32 devices in a mesh: dp: 8 (over y, x, core), expert: 4 (over z).
Axes of the slice: x: 2, y: 2, z: 4, core: 2. Of those that a mesh axis runs over, the one named last changes fastest.
Arguments:
- tokens: bfloat16 [4096, 1792], P(('dp', 'expert')), may hold values from -6 to 6
- routes: int32 [4096, 2], P(('dp', 'expert')), may hold values from 0 to 3, all different within a row; in each aligned block of 128 rows (0 to 127, 128 to 255, ...) at most 128 rows name the same one
- gates: float32 [4096, 2], P(('dp', 'expert')), may hold values from 0.25 to 1
- grad_hidden: bfloat16 [4096, 2, 512], P(('dp', 'expert')), may hold values from -4 to 4
- w_in: bfloat16 [4, 1792, 512], P('expert', 'dp'), may hold values from -0.25 to 0.25
- error: bfloat16 [8, 4, 1792, 512], P('dp', 'expert'), may hold values from -6 to 6
- q_seed: float32 [4, 512, 32], P('expert'), may hold values from -6 to 6
Outputs:
- grad_tokens: bfloat16 [4096, 1792], P(('dp', 'expert'))
- error_next: bfloat16 [8, 4, 1792, 512], P('dp', 'expert')
- weight_grad: float32 [4, 1792, 512], P('expert', 'dp')
The draws below stay inside these ranges and needn't reach their ends.
Inputs may be any that keep to these rules, and one draw needn't show every extreme that they name: `routes`: in the rows of one device no expert is named by more than 128 rows, a bound that some block reaches; the two experts of a row differ.
All inputs are finite; a program needn't handle non-finite values.
Results may differ from the reference program's by a relative error of at most 0.014.
Values may be sent and summed in bfloat16 or wider, within the bound.
A program may use at most 64 MiB of HBM per device.

```python
import math
import jax
import jax.numpy as jnp
import numpy as np
from jax import lax

D = 1792
F = 512
RANK = 32
TOK_DEV = 128
EXPERTS = 4
REPLICAS = 8
CAP = 128
TOKENS = 4096
N_DP = 8
N_EXPERT = 4


def block_scale(own_key, dims, split, smallest, high):
    level, own = 1.0, jax.random.fold_in(own_key, 6)
    for position, blocks in split:
        draws = jnp.exp(jax.random.uniform(jax.random.fold_in(own, position), (blocks,), jnp.float32, smallest / len(split), high / len(split)))
        level = level * jnp.repeat(draws, dims[position] // blocks).reshape([-1 if axis == position else 1 for axis in range(len(dims))])
    return level


def shared_out(stream_key, own, number, rows, count, top, limit, lean):
    order = jax.random.permutation(stream_key, count)
    heavy_load, usual = portions_of(count, rows * top, limit, lean, True), portions_of(count, rows * top, limit, lean, False)
    places = jnp.arange(count)

    def named(lengths, turn):
        used = int((lengths > 0).sum())
        fixed = max(1, used // 4)
        shifted = fixed + (places - fixed + turn * (used - fixed)) % max(1, count - fixed)
        return jnp.zeros((count,), jnp.int32).at[order[jnp.where(places < fixed, places, shifted)]].set(jnp.asarray(lengths, jnp.int32))

    lengths = jnp.where(number % 4 == 0, named(heavy_load, number // 4), named(usual, number - number // 4 - 1))
    mixed = jax.random.permutation(jax.random.fold_in(own, 3), count)
    source_of, sink = mixed[0:count // 2 * 2:2], mixed[1:count // 2 * 2:2]
    slack = jnp.minimum(lengths[source_of] - 1, limit - lengths[sink]) // 2
    slack = jnp.where((source_of == order[0]) | (sink == order[0]) | (lengths[sink] == 0), 0, jnp.maximum(slack, 0))
    shifted = jax.random.randint(jax.random.fold_in(own, 4), (count // 2,), 0, 1 << 20) % (slack + 1)
    lengths = lengths.at[source_of].add(-shifted).at[sink].add(shifted)
    members = jnp.searchsorted(jnp.cumsum(lengths), jnp.arange(rows * top), side="right").astype(jnp.int32)
    listing = members.reshape(top, rows).T
    listing = listing[jax.random.permutation(jax.random.fold_in(own, 1), rows)]
    turn = jax.random.randint(jax.random.fold_in(own, 2), (rows, 1), 0, top)
    return jnp.take_along_axis(listing, (jnp.arange(top)[None, :] + turn) % top, axis=1)


def portions_of(count, total, limit, lean, full):
    weights = [(1 << 20) // math.isqrt(rank ** lean) + 1 for rank in range(1, count + 1)]
    largest = limit if full else min(limit, max(-(-total // count), total * weights[0] // sum(weights)))
    least = 1 if total - largest >= count - 1 else 0
    holding, spare = [largest] + [least] * (count - 1), total - largest - least * (count - 1)
    while spare > 0:
        movable = [i for i in range(1, count) if holding[i] < largest] or [i for i in range(1, count) if holding[i] < limit]
        mass, budget = sum([weights[i] for i in movable]), spare
        for i in movable:
            more = min(limit - holding[i], max(1, budget * weights[i] // mass), spare)
            holding[i] = holding[i] + more
            spare = spare - more
    return np.array(holding)


def gaussian(rng, extent, scale, bound, pieces=(), kind=jnp.bfloat16):
    values = jax.random.normal(rng, extent, jnp.float32) * scale
    if len(pieces) > 0:
        values = block_scale(rng, extent, pieces, -0.22, 0.18) * values
    return jnp.clip(values, min=-bound, max=bound).astype(kind)


def setup_inputs(seed: int = 0) -> dict:
    arg_keys = jax.random.split(jax.random.key(seed), 8)
    tokens = gaussian(arg_keys[0], (TOKENS, D), 1.0, 6.0, ((0, 32),))
    routes_keys = jax.random.split(jax.random.fold_in(arg_keys[1], 1), TOKENS // TOK_DEV)
    routes_turns = jax.random.permutation(jax.random.fold_in(arg_keys[1], 3), TOKENS // TOK_DEV)
    routes = jax.vmap(lambda own, number: shared_out(jax.random.fold_in(arg_keys[1], 2), own, number, TOK_DEV, EXPERTS, 2, CAP, 1))(routes_keys, routes_turns).reshape((TOKENS, 2))
    gates = jnp.clip(0.25 + 0.75 * jax.random.uniform(arg_keys[2], (TOKENS, 2), jnp.float32) ** block_scale(arg_keys[2], (TOKENS, 2), ((0, 32),), -0.2, 0.2), 0.25, 1.0)
    grad_hidden = gaussian(arg_keys[3], (TOKENS, 2, F), 0.5, 4.0, ((0, 32),))
    w_in = gaussian(arg_keys[4], (EXPERTS, D, F), F ** -0.5, 0.25, ((0, 4), (1, 8)))
    error = gaussian(arg_keys[5], (REPLICAS, EXPERTS, D, F), 1.0, 6.0, ((0, 8), (1, 4)))
    q_seed = gaussian(arg_keys[6], (EXPERTS, F, RANK), 1.0, 6.0, ((0, 4),), jnp.float32)
    return dict(tokens=tokens, routes=routes, gates=gates, grad_hidden=grad_hidden, w_in=w_in, error=error, q_seed=q_seed)


highest = lax.Precision.HIGHEST

def slopes(pre_act):
    squashed = jax.nn.sigmoid(pre_act)
    return squashed * (1.0 + pre_act * (1.0 - squashed))

def gram_schmidt(factor):
    height = factor.shape[0]

    def column(ordinal, basis):
        vector = lax.dynamic_index_in_dim(basis, ordinal, 0, keepdims=False)
        vector = vector / jnp.sqrt(jnp.sum(vector * vector))
        coeffs = jnp.dot(basis, vector, precision=highest)
        beyond = (jnp.arange(height) > ordinal).astype(basis.dtype)
        basis = basis - (coeffs * beyond)[:, None] * vector[None, :]
        return lax.dynamic_update_index_in_dim(basis, vector, ordinal, 0)
    return lax.fori_loop(0, height, column, factor)

def choose_slots(chosen, expert):
    matches = chosen == expert
    slots = jnp.cumsum(matches.astype(jnp.int32)) - 1
    target = jnp.where(matches, slots, CAP).astype(jnp.int32)
    ordinal = jnp.arange(chosen.shape[0], dtype=jnp.int32)
    indices = jnp.zeros((CAP + 1,), jnp.int32).at[target].set(ordinal)[:CAP]
    filled = jnp.zeros((CAP + 1,), jnp.float32).at[target].set(1.0)[:CAP]
    return (indices, filled)

def take_rows(source, places):
    return source[places]

def add_rows(buffer, places, values):
    return buffer.at[places].add(values)

def replica_work(arrived, arrived_grad, stored, weight):
    pre_act = jnp.dot(arrived, weight, preferred_element_type=jnp.float32)
    grad_pre = (arrived_grad.astype(jnp.float32) * slopes(pre_act)).astype(jnp.bfloat16)
    weight_term = lax.dot_general(arrived, grad_pre, (((0,), (0,)), ((), ())), preferred_element_type=jnp.float32)
    grad_rows = lax.dot_general(grad_pre, weight, (((1,), (1,)), ((), ())), preferred_element_type=jnp.float32)
    return (weight_term + stored.astype(jnp.float32), grad_rows.astype(jnp.bfloat16))

def reference(tokens, routes, gates, grad_hidden, w_in, error, q_seed):
    blocks = tokens.reshape(N_DP, N_EXPERT, TOK_DEV, D)
    chosen_all = routes.reshape(N_DP, N_EXPERT, 2 * TOK_DEV)
    gate_all = gates.reshape(N_DP, N_EXPERT, 2 * TOK_DEV)
    grad_all = grad_hidden.reshape(N_DP, N_EXPERT, 2 * TOK_DEV, F)
    slot_finder = jax.vmap(jax.vmap(choose_slots, (0, None)), (0, None))
    take_twice = jax.vmap(jax.vmap(take_rows))
    add_twice = jax.vmap(jax.vmap(add_rows))
    work_all = jax.vmap(replica_work, (0, 0, 0, None))

    def per_expert(running, expert):
        indices, filled = slot_finder(chosen_all, expert)
        token_rows = indices // 2
        gate_sel = take_twice(gate_all, indices) * filled
        scaled = (take_twice(blocks, token_rows).astype(jnp.float32) * gate_sel[..., None]).astype(jnp.bfloat16)
        sent_grad = (take_twice(grad_all, indices).astype(jnp.float32) * filled[..., None]).astype(jnp.bfloat16)
        weight = w_in[expert]
        merged, grad_rows = work_all(scaled.reshape(N_DP, N_EXPERT * CAP, D), sent_grad.reshape(N_DP, N_EXPERT * CAP, F), error[:, expert], weight)
        q_start = q_seed[expert].astype(jnp.float32)
        summed = jnp.einsum('fr,ndf->rd', q_start, merged, precision=highest) / N_DP
        basis = gram_schmidt(summed)
        q_factor = jnp.einsum('rd,ndf->rf', basis, merged, precision=highest) / N_DP
        low_rank = jnp.dot(basis.T, q_factor, precision=highest)
        error_out = (merged - low_rank[None]).astype(jnp.bfloat16)
        returned = grad_rows.reshape(N_DP, N_EXPERT, CAP, D).astype(jnp.float32) * gate_sel[..., None]
        running = add_twice(running, token_rows, returned)
        return (running, (error_out, low_rank))
    initial = jnp.zeros((N_DP, N_EXPERT, TOK_DEV, D), jnp.float32)
    running, (errors, low_rank) = lax.scan(per_expert, initial, jnp.arange(EXPERTS))
    grad_tokens = running.reshape(N_DP * N_EXPERT * TOK_DEV, D).astype(jnp.bfloat16)
    return (grad_tokens, jnp.transpose(errors, (1, 0, 2, 3)), low_rank)
```

```python
import functools

import jax
import jax.numpy as jnp
from jax import lax
from jax.experimental import pallas as pl
from jax.experimental.pallas import tpu as pltpu
from jax.sharding import PartitionSpec as P

HI = lax.Precision.HIGHEST
MESH = pl.DeviceIdType.MESH
F32 = jnp.float32
BF16 = jnp.bfloat16


def slopes(pre_act):
    squashed = 1.0 / (1.0 + jnp.exp(-pre_act))
    return squashed * (1.0 + pre_act * (1.0 - squashed))


def inverse_factor(gram):
    rank = gram.shape[0]
    rows = lax.broadcasted_iota(jnp.int32, (rank, rank), 0)
    cols = lax.broadcasted_iota(jnp.int32, (rank, rank), 1)
    left = gram
    right = (rows == cols).astype(F32)
    row_id = lax.broadcasted_iota(jnp.int32, (rank, 1), 0)
    for i in range(rank):
        inv = 1.0 / jnp.sqrt(left[i : i + 1, i : i + 1])
        row_l = left[i : i + 1, :] * inv
        row_r = right[i : i + 1, :] * inv
        col = jnp.where(row_id > i, left[:, i : i + 1] * inv, 0.0)
        here = row_id == i
        left = jnp.where(here, row_l, left - col * row_l)
        right = jnp.where(here, row_r, right - col * row_r)
    return right


def kernel(dims, tok_ref, gh_ref, gate_ref, w_ref, err_hbm, qt_ref,
           gt_out, err_out, wg_out,
           tok_all, gh_all, gate_all, w_all, x_all, gp_all, err_v, merged, back, ret,
           fbuf, rsbuf, agbuf, tbuf,
           err_sem, tok_s, tok_r, gh_s, gh_r, gate_s, gate_r, w_s, w_r,
           f_s, f_r, a_s, a_r, t_s, t_r, b_s, b_r):
    E, N, rp, chunk, gather_w = dims
    z = lax.axis_index("expert")
    me = lax.axis_index("dp")
    tokens, width = tok_ref.shape
    shard = width // N
    rank = qt_ref.shape[0]
    groups = width // 128

    def other(axis, size, k):
        return lax.rem(lax.axis_index(axis) + k, size)

    def loop(size, fn, start=1):
        def step(k, c):
            fn(k)
            return c
        lax.fori_loop(start, size, step, 0)

    err_copy = pltpu.make_async_copy(err_hbm.at[0, 0], err_v, err_sem)
    err_copy.start()

    barrier = pltpu.get_barrier_semaphore()
    loop(E, lambda k: pl.semaphore_signal(
        barrier, inc=1, device_id={"expert": other("expert", E, k)}, device_id_type=MESH))
    loop(N, lambda k: pl.semaphore_signal(
        barrier, inc=1, device_id={"dp": other("dp", N, k)}, device_id_type=MESH))
    pl.semaphore_wait(barrier, E - 1 + N - 1)

    def rdma(src, dst, s, r, axis, peer):
        return pltpu.make_async_remote_copy(
            src_ref=src, dst_ref=dst, send_sem=s, recv_sem=r,
            device_id={axis: peer}, device_id_type=MESH)

    def gate_copy(p, slot, k):
        return rdma(gate_ref.at[p], gate_all.at[slot], gate_s.at[k], gate_r.at[slot], "expert", p)

    def gh_copy(p, slot, k):
        return rdma(gh_ref.at[p], gh_all.at[slot], gh_s.at[k], gh_r.at[slot], "expert", p)

    def tok_copy(j, nb, slot):
        src = tok_all.at[j]
        return rdma(src, tok_all.at[j], tok_s.at[slot], tok_r.at[j], "expert", nb)

    def w_copy(p, slot, k):
        return rdma(w_ref, w_all.at[pl.ds(pl.multiple_of(slot * shard, 16), shard)],
                    w_s.at[k], w_r.at[slot], "dp", p)

    def each(p_axis, size, copy, act):
        mine = lax.axis_index(p_axis)

        def fn(k):
            p = other(p_axis, size, k)
            if act == "start":
                copy(p, mine, k).start()
            elif act == "recv":
                copy(p, p, k).wait_recv()
            else:
                copy(p, mine, k).wait_send()
        loop(size, fn)

    def forward(s, mode):
        for d, dirn in enumerate((1, -1)):
            j = z - dirn * s
            nb = z + dirn
            inside = (j >= 0) & (j < E)
            linked = inside & (nb >= 0) & (nb < E)
            slot = d * E + s
            if mode == "first":
                @pl.when(linked)
                def _():
                    rdma(tok_ref, tok_all.at[z], tok_s.at[slot], tok_r.at[z], "expert", nb).start()
            elif mode == "relay":
                @pl.when(inside)
                def _():
                    tok_copy(j, nb, slot).wait_recv()

                @pl.when(linked)
                def _():
                    tok_copy(j, nb, slot).start()
            else:
                @pl.when(linked)
                def _():
                    tok_copy(j, nb, slot).wait_send()

    each("expert", E, gate_copy, "start")
    forward(0, "first")
    each("expert", E, gh_copy, "start")
    if gather_w:
        each("dp", N, w_copy, "start")
        w_all[pl.ds(pl.multiple_of(me * shard, 16), shard), :] = w_ref[...]
        weights = w_all
    else:
        weights = w_ref
    tok_all[z] = tok_ref[...]
    gh_all[z] = gh_ref[z]
    gate_all[z] = gate_ref[z]
    each("expert", E, gate_copy, "recv")
    forward(1, "relay")
    if gather_w:
        each("dp", N, w_copy, "recv")

    def back_copy(p, slot, k):
        return rdma(back.at[p], ret.at[slot], b_s.at[p], b_r.at[slot], "expert", p)

    def block(i, c):
        s = i // 2
        d = lax.rem(i, 2)

        @pl.when((d == 0) & (s >= 2))
        def _():
            forward(s, "relay")

        j = z - (1 - 2 * d) * s

        @pl.when((j >= 0) & (j < E) & (i != 1))
        def _():
            @pl.when(s > 0)
            def _():
                gh_copy(j, j, 0).wait_recv()
            g = jnp.transpose(gate_all[j])[:, :1]
            x = (tok_all[j].astype(F32) * g).astype(BF16)
            x_all[j] = x
            pre = jnp.dot(x, weights[...], preferred_element_type=F32)
            gp = (gh_all[j].astype(F32) * slopes(pre)).astype(BF16)
            gp_all[j] = gp
            rows = lax.dot_general(gp, weights[...], (((1,), (1,)), ((), ())),
                                   preferred_element_type=F32)
            back[j] = (rows * g).astype(BF16)

            @pl.when(s > 0)
            def _():
                back_copy(j, z, 0).start()
        return c
    lax.fori_loop(0, 2 * E, block, 0)

    err_copy.wait()
    if fbuf.shape[0] > groups * rank:
        fbuf[...] = jnp.zeros_like(fbuf)

    def merge(c):
        cols = pl.ds(pl.multiple_of(c * chunk, chunk), chunk)
        x = x_all[:, :, cols].reshape(E * tokens, chunk)
        gp = gp_all[...].reshape(E * tokens, gp_all.shape[2])
        m = lax.dot_general(x, gp, (((0,), (0,)), ((), ())), preferred_element_type=F32)
        m = m + err_v[cols, :].astype(F32)
        merged[cols, :] = m
        f = lax.dot_general(qt_ref[...], m, (((1,), (1,)), ((), ())), precision=HI,
                            preferred_element_type=F32)
        for h in range(chunk // 128):
            fbuf[pl.ds(pl.multiple_of((c * (chunk // 128) + h) * rank, rank), rank), :] = (
                f[:, h * 128 : (h + 1) * 128])
    loop(width // chunk, merge, 0)

    def f_copy(p, slot, k):
        return rdma(fbuf.at[pl.ds(pl.multiple_of(p * rp, 8), rp)], rsbuf.at[slot],
                    f_s.at[k], f_r.at[slot], "dp", p)

    def a_copy(p, slot, k):
        part = agbuf.at[pl.ds(pl.multiple_of(slot * rp, 8), rp)]
        return rdma(part, part, a_s.at[k], a_r.at[slot], "dp", p)

    def t_copy(p, slot, k):
        return rdma(tbuf.at[slot], tbuf.at[slot], t_s.at[k], t_r.at[slot], "dp", p)

    own = pl.ds(pl.multiple_of(me * rp, 8), rp)
    each("dp", N, f_copy, "start")
    rsbuf[me] = fbuf[own, :]
    each("dp", N, f_copy, "recv")
    agbuf[own, :] = jnp.sum(rsbuf[...], axis=0) * (1.0 / N)
    each("dp", N, a_copy, "start")
    each("dp", N, a_copy, "recv")
    factor = jnp.concatenate([agbuf[c * rank : (c + 1) * rank, :] for c in range(groups)], axis=1)
    gram = lax.dot_general(factor, factor, (((1,), (1,)), ((), ())), precision=HI,
                           preferred_element_type=F32)
    basis = jnp.dot(inverse_factor(gram), factor, precision=HI, preferred_element_type=F32)
    right = jnp.dot(basis, merged[...], precision=HI, preferred_element_type=F32)
    tbuf[me] = right.astype(BF16)
    each("dp", N, t_copy, "start")
    basis_t = jnp.transpose(basis)
    each("dp", N, t_copy, "recv")
    q_factor = jnp.sum(tbuf[...].astype(F32), axis=0) * (1.0 / N)

    for c in range(width // chunk):
        cols = pl.ds(c * chunk, chunk)
        low = jnp.dot(basis_t[c * chunk : (c + 1) * chunk, :], q_factor, precision=HI,
                      preferred_element_type=F32)
        err_out[0, 0, cols, :] = (merged[cols, :] - low).astype(BF16)
        merged[cols, :] = low
    wg_out[0] = merged[pl.ds(pl.multiple_of(me * shard, 8), shard), :]

    each("expert", E, back_copy, "recv")
    ret[z] = back[z]
    total = ret[0].astype(F32)
    for j in range(1, E):
        total = total + ret[j].astype(F32)
    gt_out[...] = total.astype(BF16)

    forward_first = [(0, 1), (1, -1)]
    for d, dirn in forward_first:
        nb = z + dirn

        @pl.when((nb >= 0) & (nb < E))
        def _():
            rdma(tok_ref, tok_all.at[z], tok_s.at[d * E], tok_r.at[z], "expert", nb).wait_send()
    loop(E, lambda s: forward(s, "drain"))
    each("expert", E, gate_copy, "send")
    each("expert", E, gh_copy, "send")
    if gather_w:
        each("dp", N, w_copy, "send")
    each("expert", E, back_copy, "send")
    each("dp", N, f_copy, "send")
    each("dp", N, a_copy, "send")
    each("dp", N, t_copy, "send")


def body(tokens, routes, gates, grad_hidden, w_in, error, q_seed):
    E = lax.axis_size("expert")
    N = lax.axis_size("dp")
    rows, width = tokens.shape
    hidden = grad_hidden.shape[2]
    rank = q_seed.shape[2]
    shard = width // N
    ids = jnp.arange(E, dtype=jnp.int32)
    hit0 = routes[None, :, 0] == ids[:, None]
    hit1 = routes[None, :, 1] == ids[:, None]
    gate_sel = jnp.where(hit0, gates[None, :, 0], jnp.where(hit1, gates[None, :, 1], 0.0))
    gate_sel = jnp.broadcast_to(gate_sel[:, None, :], (E, 8, rows))
    zero = jnp.zeros((), BF16)
    gh_sel = jnp.where(hit0[:, :, None], grad_hidden[None, :, 0, :],
                       jnp.where(hit1[:, :, None], grad_hidden[None, :, 1, :], zero))
    gather_w = shard % 16 == 0
    weight = w_in[0] if gather_w else lax.all_gather(w_in[0], "dp", axis=0, tiled=True)
    chunk = 256 if width % 256 == 0 else 128
    total_rows = width // 128 * rank
    rp = -(-total_rows // N)
    rp = -(-rp // 8) * 8
    dma = pltpu.SemaphoreType.DMA
    vmem = pl.BlockSpec(memory_space=pltpu.VMEM)
    return pl.pallas_call(
        functools.partial(kernel, (E, N, rp, chunk, gather_w)),
        out_shape=(
            jax.ShapeDtypeStruct((rows, width), BF16),
            jax.ShapeDtypeStruct((1, 1, width, hidden), BF16),
            jax.ShapeDtypeStruct((1, shard, hidden), F32),
        ),
        in_specs=[vmem, vmem, vmem, vmem, pl.BlockSpec(memory_space=pl.ANY), vmem],
        out_specs=(vmem, vmem, vmem),
        scratch_shapes=[
            pltpu.VMEM((E, rows, width), BF16),
            pltpu.VMEM((E, rows, hidden), BF16),
            pltpu.VMEM((E, 8, rows), F32),
            pltpu.VMEM((width if gather_w else 16, hidden), BF16),
            pltpu.VMEM((E, rows, width), BF16),
            pltpu.VMEM((E, rows, hidden), BF16),
            pltpu.VMEM((width, hidden), BF16),
            pltpu.VMEM((width, hidden), F32),
            pltpu.VMEM((E, rows, width), BF16),
            pltpu.VMEM((E, rows, width), BF16),
            pltpu.VMEM((rp * N, 128), F32),
            pltpu.VMEM((N, rp, 128), F32),
            pltpu.VMEM((rp * N, 128), F32),
            pltpu.VMEM((N, rank, hidden), BF16),
            dma(()), dma((2 * E,)), dma((E,)), dma((E,)), dma((E,)), dma((E,)), dma((E,)),
            dma((N,)), dma((N,)), dma((N,)), dma((N,)), dma((N,)), dma((N,)), dma((N,)), dma((N,)),
            dma((E,)), dma((E,)),
        ],
        compiler_params=pltpu.CompilerParams(
            collective_id=0, has_side_effects=True, vmem_limit_bytes=67043328 - (1 << 20)),
    )(tokens, gh_sel, gate_sel, weight, error, q_seed[0].T)


def solution(mesh):
    placed = (
        P(("dp", "expert"), None),
        P(("dp", "expert"), None),
        P(("dp", "expert"), None),
        P(("dp", "expert"), None, None),
        P("expert", "dp", None),
        P("dp", "expert", None, None),
        P("expert", None, None),
    )
    return jax.shard_map(
        body,
        mesh=mesh,
        in_specs=placed,
        out_specs=(
            P(("dp", "expert"), None),
            P("dp", "expert", None, None),
            P("expert", "dp", None),
        ),
        check_vma=False,
    )
```

```python
import functools

import jax
import jax.numpy as jnp
from jax import lax
from jax.experimental import pallas as pl
from jax.experimental.pallas import tpu as pltpu
from jax.sharding import PartitionSpec as P

HI = lax.Precision.HIGHEST
MESH = pl.DeviceIdType.MESH
F32 = jnp.float32
BF16 = jnp.bfloat16


def slopes(pre_act):
    squashed = 1.0 / (1.0 + jnp.exp(-pre_act))
    return squashed * (1.0 + pre_act * (1.0 - squashed))


def inverse_factor(gram):
    rank = gram.shape[0]
    rows = lax.broadcasted_iota(jnp.int32, (rank, rank), 0)
    cols = lax.broadcasted_iota(jnp.int32, (rank, rank), 1)
    left = gram
    right = (rows == cols).astype(F32)
    row_id = lax.broadcasted_iota(jnp.int32, (rank, 1), 0)
    for i in range(rank):
        inv = 1.0 / jnp.sqrt(left[i : i + 1, i : i + 1])
        row_l = left[i : i + 1, :] * inv
        row_r = right[i : i + 1, :] * inv
        col = jnp.where(row_id > i, left[:, i : i + 1] * inv, 0.0)
        here = row_id == i
        left = jnp.where(here, row_l, left - col * row_l)
        right = jnp.where(here, row_r, right - col * row_r)
    return right


def kernel(dims, tok_ref, gh_ref, gate_ref, w_ref, err_hbm, qt_ref,
           gt_out, err_out, wg_out,
           tok_all, gh_all, gate_all, w_all, x_all, gp_all, err_v, merged, back, ret,
           facc, fbuf, rsbuf, agbuf, tbuf,
           err_sem, tok_s, tok_r, gh_s, gh_r, gate_s, gate_r, w_s, w_r,
           f_s, f_r, a_s, a_r, t_s, t_r, b_s, b_r):
    E, N, rp, chunk, gather_w = dims
    z = lax.axis_index("expert")
    me = lax.axis_index("dp")
    tokens, width = tok_ref.shape
    shard = width // N
    rank = qt_ref.shape[0]
    groups = width // 128

    def other(axis, size, k):
        return lax.rem(lax.axis_index(axis) + k, size)

    def loop(size, fn, start=1):
        def step(k, c):
            fn(k)
            return c
        lax.fori_loop(start, size, step, 0)

    err_copy = pltpu.make_async_copy(err_hbm.at[0, 0], err_v, err_sem)
    err_copy.start()

    barrier = pltpu.get_barrier_semaphore()
    loop(E, lambda k: pl.semaphore_signal(
        barrier, inc=1, device_id={"expert": other("expert", E, k)}, device_id_type=MESH))
    loop(N, lambda k: pl.semaphore_signal(
        barrier, inc=1, device_id={"dp": other("dp", N, k)}, device_id_type=MESH))
    pl.semaphore_wait(barrier, E - 1 + N - 1)

    def rdma(src, dst, s, r, axis, peer):
        return pltpu.make_async_remote_copy(
            src_ref=src, dst_ref=dst, send_sem=s, recv_sem=r,
            device_id={axis: peer}, device_id_type=MESH)

    def gate_copy(p, slot, k):
        return rdma(gate_ref.at[p], gate_all.at[slot], gate_s.at[k], gate_r.at[slot], "expert", p)

    def gh_copy(p, slot, k):
        return rdma(gh_ref.at[p], gh_all.at[slot], gh_s.at[k], gh_r.at[slot], "expert", p)

    def tok_copy(j, nb, slot):
        src = tok_all.at[j]
        return rdma(src, tok_all.at[j], tok_s.at[slot], tok_r.at[j], "expert", nb)

    def w_copy(p, slot, k):
        return rdma(w_ref, w_all.at[pl.ds(pl.multiple_of(slot * shard, 16), shard)],
                    w_s.at[k], w_r.at[slot], "dp", p)

    def each(p_axis, size, copy, act):
        mine = lax.axis_index(p_axis)

        def fn(k):
            p = other(p_axis, size, k)
            if act == "start":
                copy(p, mine, k).start()
            elif act == "recv":
                copy(p, p, k).wait_recv()
            else:
                copy(p, mine, k).wait_send()
        loop(size, fn)

    def forward(s, mode):
        for d, dirn in enumerate((1, -1)):
            j = z - dirn * s
            nb = z + dirn
            inside = (j >= 0) & (j < E)
            linked = inside & (nb >= 0) & (nb < E)
            slot = d * E + s
            if mode == "first":
                @pl.when(linked)
                def _():
                    rdma(tok_ref, tok_all.at[z], tok_s.at[slot], tok_r.at[z], "expert", nb).start()
            elif mode == "relay":
                @pl.when(inside)
                def _():
                    tok_copy(j, nb, slot).wait_recv()

                @pl.when(linked)
                def _():
                    tok_copy(j, nb, slot).start()
            else:
                @pl.when(linked)
                def _():
                    tok_copy(j, nb, slot).wait_send()

    each("expert", E, gate_copy, "start")
    forward(0, "first")
    each("expert", E, gh_copy, "start")
    if gather_w:
        each("dp", N, w_copy, "start")
        w_all[pl.ds(pl.multiple_of(me * shard, 16), shard), :] = w_ref[...]
        weights = w_all
    else:
        weights = w_ref
    tok_all[z] = tok_ref[...]
    gh_all[z] = gh_ref[z]
    gate_all[z] = gate_ref[z]
    err_copy.wait()

    def err_factor(c):
        cols = pl.ds(pl.multiple_of(c * chunk, chunk), chunk)
        facc[:, cols] = lax.dot_general(
            qt_ref[...], err_v[cols, :].astype(F32), (((1,), (1,)), ((), ())), precision=HI,
            preferred_element_type=F32)
    loop(width // chunk, err_factor, 0)
    each("expert", E, gate_copy, "recv")
    forward(1, "relay")
    if gather_w:
        each("dp", N, w_copy, "recv")

    def back_copy(d):
        dirn = jnp.where(d > z, 1, -1)
        direct = (d - z) * dirn == E - 1
        slot = jnp.where(direct, E + 1, jnp.where((d == z - 1), E, d))
        return rdma(back.at[d], ret.at[slot], b_s.at[d], b_r.at[slot], "expert",
                    jnp.where(direct, d, z + dirn))

    def back_wait(slot):
        rdma(back.at[0], ret.at[slot], b_s.at[0], b_r.at[slot], "expert",
             other("expert", E, 1)).wait_recv()

    def first_right(d):
        return jnp.where(d == E - 1, 1, 0)

    def first_left(d):
        return jnp.where(d == 0, E - 2, E - 1)

    def add_back(d, slot):
        back[d] = (back[d].astype(F32) + ret[slot].astype(F32)).astype(BF16)

    def block(i, c):
        s = i // 2
        d = lax.rem(i, 2)

        @pl.when((d == 0) & (s >= 2))
        def _():
            forward(s, "relay")

        j = z - (1 - 2 * d) * s

        @pl.when((j >= 0) & (j < E) & (i != 1))
        def _():
            @pl.when(s > 0)
            def _():
                gh_copy(j, j, 0).wait_recv()
            g = jnp.transpose(gate_all[j])[:, :1]
            x = (tok_all[j].astype(F32) * g).astype(BF16)
            x_all[j] = x
            pre = jnp.dot(x, weights[...], preferred_element_type=F32)
            gp = (gh_all[j].astype(F32) * slopes(pre)).astype(BF16)
            gp_all[j] = gp
            seen = lax.dot_general(gp.astype(F32), qt_ref[...], (((1,), (1,)), ((), ())),
                                   precision=HI, preferred_element_type=F32)
            facc[...] += lax.dot_general(seen, x.astype(F32), (((0,), (0,)), ((), ())),
                                         precision=HI, preferred_element_type=F32)
            rows = lax.dot_general(gp, weights[...], (((1,), (1,)), ((), ())),
                                   preferred_element_type=F32)
            back[j] = (rows * g).astype(BF16)

            @pl.when(((j > z) & (z <= first_right(j))) | ((j < z) & (z >= first_left(j))))
            def _():
                back_copy(j).start()
        return c
    lax.fori_loop(0, 2 * E, block, 0)

    if fbuf.shape[0] > groups * rank:
        fbuf[...] = jnp.zeros_like(fbuf)
    for c in range(groups):
        fbuf[c * rank : (c + 1) * rank, :] = facc[:, c * 128 : (c + 1) * 128]

    def f_copy(p, slot, k):
        return rdma(fbuf.at[pl.ds(pl.multiple_of(p * rp, 8), rp)], rsbuf.at[slot],
                    f_s.at[k], f_r.at[slot], "dp", p)

    def a_copy(p, slot, k):
        part = agbuf.at[pl.ds(pl.multiple_of(slot * rp, 8), rp)]
        return rdma(part, part, a_s.at[k], a_r.at[slot], "dp", p)

    def t_copy(p, slot, k):
        return rdma(tbuf.at[slot], tbuf.at[slot], t_s.at[k], t_r.at[slot], "dp", p)

    own = pl.ds(pl.multiple_of(me * rp, 8), rp)
    each("dp", N, f_copy, "start")
    rsbuf[me] = fbuf[own, :]
    def relay_right(d):
        @pl.when((d > z) & (z > first_right(d)))
        def _():
            back_wait(d)
            add_back(d, d)
            back_copy(d).start()
    loop(E, relay_right, 0)

    def relay_left(d):
        @pl.when((d < z) & (z < first_left(d)))
        def _():
            back_wait(d)
            add_back(d, d)
            back_copy(d).start()
    loop(E, relay_left, 0)

    def merge(c):
        cols = pl.ds(pl.multiple_of(c * chunk, chunk), chunk)
        x = x_all[:, :, cols].reshape(E * tokens, chunk)
        gp = gp_all[...].reshape(E * tokens, gp_all.shape[2])
        m = lax.dot_general(x, gp, (((0,), (0,)), ((), ())), preferred_element_type=F32)
        m = m + err_v[cols, :].astype(F32)
        merged[cols, :] = m
    loop(width // chunk, merge, 0)

    each("dp", N, f_copy, "recv")
    agbuf[own, :] = jnp.sum(rsbuf[...], axis=0) * (1.0 / N)
    each("dp", N, a_copy, "start")
    each("dp", N, a_copy, "recv")
    factor = jnp.concatenate([agbuf[c * rank : (c + 1) * rank, :] for c in range(groups)], axis=1)
    gram = lax.dot_general(factor, factor, (((1,), (1,)), ((), ())), precision=HI,
                           preferred_element_type=F32)
    basis = jnp.dot(inverse_factor(gram), factor, precision=HI, preferred_element_type=F32)
    right = jnp.dot(basis, merged[...], precision=HI, preferred_element_type=F32)
    tbuf[me] = right.astype(BF16)
    each("dp", N, t_copy, "start")
    basis_t = jnp.transpose(basis)
    each("dp", N, t_copy, "recv")
    q_factor = jnp.sum(tbuf[...].astype(F32), axis=0) * (1.0 / N)

    for c in range(width // chunk):
        cols = pl.ds(c * chunk, chunk)
        low = jnp.dot(basis_t[c * chunk : (c + 1) * chunk, :], q_factor, precision=HI,
                      preferred_element_type=F32)
        err_out[0, 0, cols, :] = (merged[cols, :] - low).astype(BF16)
        merged[cols, :] = low
    wg_out[0] = merged[pl.ds(pl.multiple_of(me * shard, 8), shard), :]

    @pl.when(z > first_right(z))
    def _():
        back_wait(z)
        add_back(z, z)

    @pl.when(z < first_left(z))
    def _():
        back_wait(E)
        add_back(z, E)

    @pl.when((z == 0) | (z == E - 1))
    def _():
        back_wait(E + 1)
        add_back(z, E + 1)
    gt_out[...] = back[z]

    forward_first = [(0, 1), (1, -1)]
    for d, dirn in forward_first:
        nb = z + dirn

        @pl.when((nb >= 0) & (nb < E))
        def _():
            rdma(tok_ref, tok_all.at[z], tok_s.at[d * E], tok_r.at[z], "expert", nb).wait_send()
    loop(E, lambda s: forward(s, "drain"))
    each("expert", E, gate_copy, "send")
    each("expert", E, gh_copy, "send")
    if gather_w:
        each("dp", N, w_copy, "send")
    loop(E, lambda k: back_copy(other("expert", E, k)).wait_send())
    each("dp", N, f_copy, "send")
    each("dp", N, a_copy, "send")
    each("dp", N, t_copy, "send")


def body(tokens, routes, gates, grad_hidden, w_in, error, q_seed):
    E = lax.axis_size("expert")
    N = lax.axis_size("dp")
    rows, width = tokens.shape
    hidden = grad_hidden.shape[2]
    rank = q_seed.shape[2]
    shard = width // N
    ids = jnp.arange(E, dtype=jnp.int32)
    hit0 = routes[None, :, 0] == ids[:, None]
    hit1 = routes[None, :, 1] == ids[:, None]
    gate_sel = jnp.where(hit0, gates[None, :, 0], jnp.where(hit1, gates[None, :, 1], 0.0))
    gate_sel = jnp.broadcast_to(gate_sel[:, None, :], (E, 8, rows))
    zero = jnp.zeros((), BF16)
    gh_sel = jnp.where(hit0[:, :, None], grad_hidden[None, :, 0, :],
                       jnp.where(hit1[:, :, None], grad_hidden[None, :, 1, :], zero))
    gather_w = shard % 16 == 0
    weight = w_in[0] if gather_w else lax.all_gather(w_in[0], "dp", axis=0, tiled=True)
    chunk = 256 if width % 256 == 0 else 128
    total_rows = width // 128 * rank
    rp = -(-total_rows // N)
    rp = -(-rp // 8) * 8
    room = (4 * E + 3) * rows * width * 2 + 3 * E * rows * hidden * 2 + 13 * width * hidden + (12 << 20)
    dma = pltpu.SemaphoreType.DMA
    vmem = pl.BlockSpec(memory_space=pltpu.VMEM)
    return pl.pallas_call(
        functools.partial(kernel, (E, N, rp, chunk, gather_w)),
        out_shape=(
            jax.ShapeDtypeStruct((rows, width), BF16),
            jax.ShapeDtypeStruct((1, 1, width, hidden), BF16),
            jax.ShapeDtypeStruct((1, shard, hidden), F32),
        ),
        in_specs=[vmem, vmem, vmem, vmem, pl.BlockSpec(memory_space=pl.ANY), vmem],
        out_specs=(vmem, vmem, vmem),
        scratch_shapes=[
            pltpu.VMEM((E, rows, width), BF16),
            pltpu.VMEM((E, rows, hidden), BF16),
            pltpu.VMEM((E, 8, rows), F32),
            pltpu.VMEM((width if gather_w else 16, hidden), BF16),
            pltpu.VMEM((E, rows, width), BF16),
            pltpu.VMEM((E, rows, hidden), BF16),
            pltpu.VMEM((width, hidden), BF16),
            pltpu.VMEM((width, hidden), F32),
            pltpu.VMEM((E, rows, width), BF16),
            pltpu.VMEM((E + 2, rows, width), BF16),
            pltpu.VMEM((rank, width), F32),
            pltpu.VMEM((rp * N, 128), F32),
            pltpu.VMEM((N, rp, 128), F32),
            pltpu.VMEM((rp * N, 128), F32),
            pltpu.VMEM((N, rank, hidden), BF16),
            dma(()), dma((2 * E,)), dma((E,)), dma((E,)), dma((E,)), dma((E,)), dma((E,)),
            dma((N,)), dma((N,)), dma((N,)), dma((N,)), dma((N,)), dma((N,)), dma((N,)), dma((N,)),
            dma((E,)), dma((E + 2,)),
        ],
        compiler_params=pltpu.CompilerParams(
            collective_id=0, has_side_effects=True, vmem_limit_bytes=min(room, 67043328 - (1 << 20))),
    )(tokens, gh_sel, gate_sel, weight, error, q_seed[0].T)


def solution(mesh):
    placed = (
        P(("dp", "expert"), None),
        P(("dp", "expert"), None),
        P(("dp", "expert"), None),
        P(("dp", "expert"), None, None),
        P("expert", "dp", None),
        P("dp", "expert", None, None),
        P("expert", None, None),
    )
    return jax.shard_map(
        body,
        mesh=mesh,
        in_specs=placed,
        out_specs=(
            P(("dp", "expert"), None),
            P("dp", "expert", None, None),
            P("expert", "dp", None),
        ),
        check_vma=False,
    )
```

```python
import functools

import jax
import jax.numpy as jnp
from jax import lax
from jax.experimental import pallas as pl
from jax.experimental.pallas import tpu as pltpu
from jax.sharding import PartitionSpec as P

HI = lax.Precision.HIGHEST
MESH = pl.DeviceIdType.MESH
F32 = jnp.float32
BF16 = jnp.bfloat16


def slopes(pre_act):
    squashed = 1.0 / (1.0 + jnp.exp(-pre_act))
    return squashed * (1.0 + pre_act * (1.0 - squashed))


def inverse_factor(gram):
    rank = gram.shape[0]
    rows = lax.broadcasted_iota(jnp.int32, (rank, rank), 0)
    cols = lax.broadcasted_iota(jnp.int32, (rank, rank), 1)
    left = gram
    right = (rows == cols).astype(F32)
    row_id = lax.broadcasted_iota(jnp.int32, (rank, 1), 0)
    for i in range(rank - 1):
        scale = 1.0 / left[i : i + 1, i : i + 1]
        col = jnp.where(row_id > i, left[:, i : i + 1], 0.0)
        row_l = left[i : i + 1, :] * scale
        row_r = right[i : i + 1, :] * scale
        left = left - col * row_l
        right = right - col * row_r
    pivots = jnp.sum(jnp.where(rows == cols, left, 0.0), axis=1, keepdims=True)
    return right * (1.0 / jnp.sqrt(pivots))


def kernel(dims, tok_ref, gh_ref, gate_ref, w_ref, err_hbm, qt_ref,
           gt_out, err_out, wg_out,
           tok_all, gh_all, gate_all, w_all, x_all, gp_all, err_v, merged, back, ret,
           facc, fbuf, rsbuf, agbuf, tbuf,
           err_sem, tok_s, tok_r, gh_s, gh_r, gate_s, gate_r, w_s, w_r,
           f_s, f_r, a_s, a_r, t_s, t_r, b_s, b_r):
    E, N, rp, chunk, gather_w = dims
    z = lax.axis_index("expert")
    me = lax.axis_index("dp")
    tokens, width = tok_ref.shape
    shard = width // N
    rank = qt_ref.shape[0]
    groups = width // 128

    def other(axis, size, k):
        return lax.rem(lax.axis_index(axis) + k, size)

    def loop(size, fn, start=1):
        def step(k, c):
            fn(k)
            return c
        lax.fori_loop(start, size, step, 0)

    err_copy = pltpu.make_async_copy(err_hbm.at[0, 0], err_v, err_sem)
    err_copy.start()

    barrier = pltpu.get_barrier_semaphore()
    loop(E, lambda k: pl.semaphore_signal(
        barrier, inc=1, device_id={"expert": other("expert", E, k)}, device_id_type=MESH))
    loop(N, lambda k: pl.semaphore_signal(
        barrier, inc=1, device_id={"dp": other("dp", N, k)}, device_id_type=MESH))
    pl.semaphore_wait(barrier, E - 1 + N - 1)

    def rdma(src, dst, s, r, axis, peer):
        return pltpu.make_async_remote_copy(
            src_ref=src, dst_ref=dst, send_sem=s, recv_sem=r,
            device_id={axis: peer}, device_id_type=MESH)

    def gate_copy(p, slot, k):
        return rdma(gate_ref.at[p], gate_all.at[slot], gate_s.at[k], gate_r.at[slot], "expert", p)

    def gh_copy(p, slot, k):
        return rdma(gh_ref.at[p], gh_all.at[slot], gh_s.at[k], gh_r.at[slot], "expert", p)

    def tok_copy(j, nb, slot):
        src = tok_all.at[j]
        return rdma(src, tok_all.at[j], tok_s.at[slot], tok_r.at[j], "expert", nb)

    def w_copy(p, slot, k):
        return rdma(w_ref, w_all.at[pl.ds(pl.multiple_of(slot * shard, 16), shard)],
                    w_s.at[k], w_r.at[slot], "dp", p)

    def each(p_axis, size, copy, act):
        mine = lax.axis_index(p_axis)

        def fn(k):
            p = other(p_axis, size, k)
            if act == "start":
                copy(p, mine, k).start()
            elif act == "recv":
                copy(p, p, k).wait_recv()
            else:
                copy(p, mine, k).wait_send()
        loop(size, fn)

    def forward(s, mode):
        for d, dirn in enumerate((1, -1)):
            j = z - dirn * s
            nb = z + dirn
            inside = (j >= 0) & (j < E)
            linked = inside & (nb >= 0) & (nb < E)
            slot = d * E + s
            if mode == "first":
                @pl.when(linked)
                def _():
                    rdma(tok_ref, tok_all.at[z], tok_s.at[slot], tok_r.at[z], "expert", nb).start()
            elif mode == "relay":
                @pl.when(inside)
                def _():
                    tok_copy(j, nb, slot).wait_recv()

                @pl.when(linked)
                def _():
                    tok_copy(j, nb, slot).start()
            else:
                @pl.when(linked)
                def _():
                    tok_copy(j, nb, slot).wait_send()

    each("expert", E, gate_copy, "start")
    forward(0, "first")
    each("expert", E, gh_copy, "start")
    if gather_w:
        each("dp", N, w_copy, "start")
        w_all[pl.ds(pl.multiple_of(me * shard, 16), shard), :] = w_ref[...]
        weights = w_all
    else:
        weights = w_ref
    tok_all[z] = tok_ref[...]
    gh_all[z] = gh_ref[z]
    gate_all[z] = gate_ref[z]
    err_copy.wait()

    def err_factor(c):
        cols = pl.ds(pl.multiple_of(c * chunk, chunk), chunk)
        facc[:, cols] = lax.dot_general(
            qt_ref[...], err_v[cols, :].astype(F32), (((1,), (1,)), ((), ())), precision=HI,
            preferred_element_type=F32)
    loop(width // chunk, err_factor, 0)
    each("expert", E, gate_copy, "recv")
    forward(1, "relay")
    if gather_w:
        each("dp", N, w_copy, "recv")

    def back_copy(d):
        dirn = jnp.where(d > z, 1, -1)
        direct = (d - z) * dirn == E - 1
        slot = jnp.where(direct, E + 1, jnp.where((d == z - 1), E, d))
        return rdma(back.at[d], ret.at[slot], b_s.at[d], b_r.at[slot], "expert",
                    jnp.where(direct, d, z + dirn))

    def back_wait(slot):
        rdma(back.at[0], ret.at[slot], b_s.at[0], b_r.at[slot], "expert",
             other("expert", E, 1)).wait_recv()

    def first_right(d):
        return jnp.where(d == E - 1, 1, 0)

    def first_left(d):
        return jnp.where(d == 0, E - 2, E - 1)

    def add_back(d, slot):
        back[d] = (back[d].astype(F32) + ret[slot].astype(F32)).astype(BF16)

    def block(i, c):
        s = i // 2
        d = lax.rem(i, 2)

        @pl.when((d == 0) & (s >= 2))
        def _():
            forward(s, "relay")

        j = z - (1 - 2 * d) * s

        @pl.when((j >= 0) & (j < E) & (i != 1))
        def _():
            @pl.when(s > 0)
            def _():
                gh_copy(j, j, 0).wait_recv()
            g = jnp.transpose(gate_all[j])[:, :1]
            x = (tok_all[j].astype(F32) * g).astype(BF16)
            x_all[j] = x
            pre = jnp.dot(x, weights[...], preferred_element_type=F32)
            gp = (gh_all[j].astype(F32) * slopes(pre)).astype(BF16)
            gp_all[j] = gp
            seen = lax.dot_general(gp.astype(F32), qt_ref[...], (((1,), (1,)), ((), ())),
                                   precision=HI, preferred_element_type=F32)
            facc[...] += lax.dot_general(seen, x.astype(F32), (((0,), (0,)), ((), ())),
                                         precision=HI, preferred_element_type=F32)
            rows = lax.dot_general(gp, weights[...], (((1,), (1,)), ((), ())),
                                   preferred_element_type=F32)
            back[j] = (rows * g).astype(BF16)

            @pl.when(((j > z) & (z <= first_right(j))) | ((j < z) & (z >= first_left(j))))
            def _():
                back_copy(j).start()
        return c
    lax.fori_loop(0, 2 * E, block, 0)

    if fbuf.shape[0] > groups * rank:
        fbuf[...] = jnp.zeros_like(fbuf)
    for c in range(groups):
        fbuf[c * rank : (c + 1) * rank, :] = facc[:, c * 128 : (c + 1) * 128]

    def f_copy(p, slot, k):
        return rdma(fbuf.at[pl.ds(pl.multiple_of(p * rp, 8), rp)], rsbuf.at[slot],
                    f_s.at[k], f_r.at[slot], "dp", p)

    def a_copy(p, slot, k):
        part = agbuf.at[pl.ds(pl.multiple_of(slot * rp, 8), rp)]
        return rdma(part, part, a_s.at[k], a_r.at[slot], "dp", p)

    def t_copy(p, slot, k):
        return rdma(tbuf.at[slot], tbuf.at[slot], t_s.at[k], t_r.at[slot], "dp", p)

    own = pl.ds(pl.multiple_of(me * rp, 8), rp)
    each("dp", N, f_copy, "start")
    rsbuf[me] = fbuf[own, :]
    def relay_right(d):
        @pl.when((d > z) & (z > first_right(d)))
        def _():
            back_wait(d)
            add_back(d, d)
            back_copy(d).start()
    loop(E, relay_right, 0)

    def relay_left(d):
        @pl.when((d < z) & (z < first_left(d)))
        def _():
            back_wait(d)
            add_back(d, d)
            back_copy(d).start()
    loop(E, relay_left, 0)

    def merge(c):
        cols = pl.ds(pl.multiple_of(c * chunk, chunk), chunk)
        x = x_all[:, :, cols].reshape(E * tokens, chunk)
        gp = gp_all[...].reshape(E * tokens, gp_all.shape[2])
        m = lax.dot_general(x, gp, (((0,), (0,)), ((), ())), preferred_element_type=F32)
        m = m + err_v[cols, :].astype(F32)
        merged[cols, :] = m
    loop(width // chunk, merge, 0)

    each("dp", N, f_copy, "recv")
    agbuf[own, :] = jnp.sum(rsbuf[...], axis=0) * (1.0 / N)
    each("dp", N, a_copy, "start")
    each("dp", N, a_copy, "recv")
    factor = jnp.concatenate([agbuf[c * rank : (c + 1) * rank, :] for c in range(groups)], axis=1)
    gram = lax.dot_general(factor, factor, (((1,), (1,)), ((), ())), precision=HI,
                           preferred_element_type=F32)
    basis = jnp.dot(inverse_factor(gram), factor, precision=HI, preferred_element_type=F32)
    right = jnp.dot(basis.astype(BF16), merged[...].astype(BF16), preferred_element_type=F32)
    tbuf[me] = right.astype(BF16)
    each("dp", N, t_copy, "start")
    basis_t = jnp.transpose(basis).astype(BF16)
    each("dp", N, t_copy, "recv")
    q_factor = (jnp.sum(tbuf[...].astype(F32), axis=0) * (1.0 / N)).astype(BF16)

    for c in range(width // chunk):
        cols = pl.ds(c * chunk, chunk)
        low = jnp.dot(basis_t[c * chunk : (c + 1) * chunk, :], q_factor,
                      preferred_element_type=F32)
        err_out[0, 0, cols, :] = (merged[cols, :] - low).astype(BF16)
        merged[cols, :] = low
    wg_out[0] = merged[pl.ds(pl.multiple_of(me * shard, 8), shard), :]

    @pl.when(z > first_right(z))
    def _():
        back_wait(z)
        add_back(z, z)

    @pl.when(z < first_left(z))
    def _():
        back_wait(E)
        add_back(z, E)

    @pl.when((z == 0) | (z == E - 1))
    def _():
        back_wait(E + 1)
        add_back(z, E + 1)
    gt_out[...] = back[z]

    forward_first = [(0, 1), (1, -1)]
    for d, dirn in forward_first:
        nb = z + dirn

        @pl.when((nb >= 0) & (nb < E))
        def _():
            rdma(tok_ref, tok_all.at[z], tok_s.at[d * E], tok_r.at[z], "expert", nb).wait_send()
    loop(E, lambda s: forward(s, "drain"))
    each("expert", E, gate_copy, "send")
    each("expert", E, gh_copy, "send")
    if gather_w:
        each("dp", N, w_copy, "send")
    loop(E, lambda k: back_copy(other("expert", E, k)).wait_send())
    each("dp", N, f_copy, "send")
    each("dp", N, a_copy, "send")
    each("dp", N, t_copy, "send")


def body(tokens, routes, gates, grad_hidden, w_in, error, q_seed):
    E = lax.axis_size("expert")
    N = lax.axis_size("dp")
    rows, width = tokens.shape
    hidden = grad_hidden.shape[2]
    rank = q_seed.shape[2]
    shard = width // N
    ids = jnp.arange(E, dtype=jnp.int32)
    hit0 = routes[None, :, 0] == ids[:, None]
    hit1 = routes[None, :, 1] == ids[:, None]
    gate_sel = jnp.where(hit0, gates[None, :, 0], jnp.where(hit1, gates[None, :, 1], 0.0))
    gate_sel = jnp.broadcast_to(gate_sel[:, None, :], (E, 8, rows))
    zero = jnp.zeros((), BF16)
    gh_sel = jnp.where(hit0[:, :, None], grad_hidden[None, :, 0, :],
                       jnp.where(hit1[:, :, None], grad_hidden[None, :, 1, :], zero))
    gather_w = shard % 16 == 0
    weight = w_in[0] if gather_w else lax.all_gather(w_in[0], "dp", axis=0, tiled=True)
    chunk = 256 if width % 256 == 0 else 128
    total_rows = width // 128 * rank
    rp = -(-total_rows // N)
    rp = -(-rp // 8) * 8
    room = (4 * E + 3) * rows * width * 2 + 3 * E * rows * hidden * 2 + 13 * width * hidden + (12 << 20)
    dma = pltpu.SemaphoreType.DMA
    vmem = pl.BlockSpec(memory_space=pltpu.VMEM)
    return pl.pallas_call(
        functools.partial(kernel, (E, N, rp, chunk, gather_w)),
        out_shape=(
            jax.ShapeDtypeStruct((rows, width), BF16),
            jax.ShapeDtypeStruct((1, 1, width, hidden), BF16),
            jax.ShapeDtypeStruct((1, shard, hidden), F32),
        ),
        in_specs=[vmem, vmem, vmem, vmem, pl.BlockSpec(memory_space=pl.ANY), vmem],
        out_specs=(vmem, vmem, vmem),
        scratch_shapes=[
            pltpu.VMEM((E, rows, width), BF16),
            pltpu.VMEM((E, rows, hidden), BF16),
            pltpu.VMEM((E, 8, rows), F32),
            pltpu.VMEM((width if gather_w else 16, hidden), BF16),
            pltpu.VMEM((E, rows, width), BF16),
            pltpu.VMEM((E, rows, hidden), BF16),
            pltpu.VMEM((width, hidden), BF16),
            pltpu.VMEM((width, hidden), F32),
            pltpu.VMEM((E, rows, width), BF16),
            pltpu.VMEM((E + 2, rows, width), BF16),
            pltpu.VMEM((rank, width), F32),
            pltpu.VMEM((rp * N, 128), F32),
            pltpu.VMEM((N, rp, 128), F32),
            pltpu.VMEM((rp * N, 128), F32),
            pltpu.VMEM((N, rank, hidden), BF16),
            dma(()), dma((2 * E,)), dma((E,)), dma((E,)), dma((E,)), dma((E,)), dma((E,)),
            dma((N,)), dma((N,)), dma((N,)), dma((N,)), dma((N,)), dma((N,)), dma((N,)), dma((N,)),
            dma((E,)), dma((E + 2,)),
        ],
        compiler_params=pltpu.CompilerParams(
            collective_id=0, has_side_effects=True, vmem_limit_bytes=min(room, 67043328 - (1 << 20))),
    )(tokens, gh_sel, gate_sel, weight, error, q_seed[0].T)


def solution(mesh):
    placed = (
        P(("dp", "expert"), None),
        P(("dp", "expert"), None),
        P(("dp", "expert"), None),
        P(("dp", "expert"), None, None),
        P("expert", "dp", None),
        P("dp", "expert", None, None),
        P("expert", None, None),
    )
    return jax.shard_map(
        body,
        mesh=mesh,
        in_specs=placed,
        out_specs=(
            P(("dp", "expert"), None),
            P("dp", "expert", None, None),
            P("expert", "dp", None),
        ),
        check_vma=False,
    )
```
